32 devices in a mesh: row: 4 (over y, x), col: 8 (over z, core).
Axes of the slice: x: 2, y: 2, z: 4, core: 2. Of those that a mesh axis runs over, the one named last changes fastest.
Arguments:
- integrals: bfloat16 [2400, 2400, 256], P('row', 'col'), may hold values from -6 to 6
- occ_coef: bfloat16 [2400, 96], P('row'), may hold values from -0.125 to 0.125
- virt_coef: bfloat16 [2400, 2304], P('col'), may hold values from -0.125 to 0.125
- pair_index: int32 [256], replicated, may hold values from 0 to 255, each once
Outputs:
- transformed: bfloat16 [96, 2304, 256], P('row', 'col')
The draws below stay inside these ranges and needn't reach their ends.
Inputs may be any that keep to these rules, and one draw needn't show every extreme that they name: pair_index holds each of 0 to 255 once.
All inputs are finite; a program needn't handle non-finite values.
Results may differ from the reference program's by a relative error of at most 0.0049.
Values may be sent and summed in bfloat16 or wider, within the bound.
A program may use at most 192 MiB of HBM per device.

```python
import jax
import jax.numpy as jnp
from jax import lax

O = 96
V = 2304
N = 2400
P_SIZE = 256


def block_scale(stream_key, shape, pieces, low, top_value):
    level = 1.0
    for position, blocks in pieces:
        heights = jax.random.uniform(jax.random.fold_in(jax.random.fold_in(stream_key, 6), position), (blocks,), jnp.float32, low / len(pieces), top_value / len(pieces))
        level = level * jnp.repeat(jnp.exp(heights), shape[position] // blocks).reshape((-1,) + (1,) * (len(shape) - 1 - position))
    return level


def centred(rng, shape, deviation, reach, shards=(), dtype=jnp.bfloat16):
    level = block_scale(rng, shape, shards, -0.22, 0.18) if shards else 1.0
    drawn = jax.random.normal(rng, shape, jnp.float32) * deviation * level
    return jnp.minimum(jnp.maximum(drawn, -reach), reach).astype(dtype)


def setup_inputs(seed: int = 0) -> dict:
    arg_keys = jax.random.split(jax.random.key(seed), 5)
    integrals = centred(arg_keys[0], (N, N, P_SIZE), 1.0, 6.0, ((0, 4), (1, 8)))
    occ_coef = centred(arg_keys[1], (N, O), N ** -0.5, 0.125, ((0, 4),))
    virt_coef = centred(arg_keys[2], (N, V), N ** -0.5, 0.125, ((0, 8),))
    pair_index = jax.random.permutation(arg_keys[3], P_SIZE).astype(jnp.int32)
    return {"integrals": integrals, "occ_coef": occ_coef, "virt_coef": virt_coef, "pair_index": pair_index}


def reference(integrals, occ_coef, virt_coef, pair_index):
    def one_pair(pair_block):
        half_rows = jnp.dot(occ_coef.T, pair_block, preferred_element_type=jnp.float32).astype(jnp.bfloat16)
        return jnp.dot(half_rows, virt_coef, preferred_element_type=jnp.float32).astype(jnp.bfloat16)

    slab_rows = lax.map(one_pair, jnp.moveaxis(integrals, 2, 0))
    chosen = jnp.take(slab_rows, pair_index.astype(jnp.int32), axis=0)
    return jnp.moveaxis(chosen, 0, 2)
```

```python
import functools

import jax
import jax.numpy as jnp
from jax import lax
from jax.experimental import pallas as pl
from jax.experimental.pallas import tpu as pltpu
from jax.sharding import PartitionSpec as P

MESH = pl.DeviceIdType.MESH
F32 = jnp.float32
BF16 = jnp.bfloat16

LANES = 128
GROUP = 8
STEP = 16
SIDES = 2
LAG_A = 2
LAG_B = 3
LAG_S = 2


def kernel(
    dims,
    x_hbm, occ_ref, vt_hbm, out_hbm,
    ibuf, part, ra, rb, half, vr, qs, qr, fsum,
    i_sem, a_send, a_recv, b_send, b_recv, own_send, own_recv, fw_send, fw_recv,
    q_send, q_recv, o_send, o_recv, l_sem, v_send, v_recv, v_loc,
):
    nus, steps, blocks, granules = dims
    padded = steps * STEP
    per_block = granules * steps
    total = blocks * per_block
    pairs = GROUP // 2
    units = GROUP
    rows_step = STEP * GROUP

    row, col = lax.axis_index("row"), lax.axis_index("col")
    y, x = row // 2, row % 2
    z, c = col // 2, col % 2
    xn, yn, dg = row + 1 - 2 * x, row + 2 - 4 * y, 3 - row
    inner_i = (z % 2 + z // 2) % 2
    inner = inner_i == 1
    outer = inner_i == 0
    zp = z + 1 - 2 * (z % 2)
    zm = 3 - z
    zmp = zm + 1 - 2 * (zm % 2)
    core_col = col + 1 - 2 * c
    pair_col = zp * 2 + c
    mid_col = zm * 2 + c
    q = (z % 2) * 2 + c
    qp = (z % 2) * 2 + 1 - c
    qo = (zp % 2) * 2 + c
    far = (1 - z // 2) * 2
    near = (z // 2) * 2

    def rcopy(src, dst, ssem, rsem, dev):
        return pltpu.make_async_remote_copy(
            src_ref=src, dst_ref=dst, send_sem=ssem, recv_sem=rsem, device_id=dev, device_id_type=MESH
        )

    barrier = pltpu.get_barrier_semaphore()
    peers = (
        (xn, col), (yn, col), (row, core_col), (row, pair_col), (row, zp * 2 + 1 - c), (row, mid_col),
    )
    for dev in peers:
        pl.semaphore_signal(barrier, inc=1, device_id=dev, device_id_type=MESH)
    pl.semaphore_wait(barrier, len(peers))

    def place(s):
        h = s // per_block
        rem = s % per_block
        return h, rem // steps, rem % steps

    def rows_of(k):
        return pl.ds(pl.multiple_of(k * rows_step, rows_step), rows_step)

    def chunk(j):
        h, k = j // steps, j % steps
        base = jnp.minimum(k * STEP, nus - STEP)
        return pltpu.make_async_copy(
            x_hbm.at[pl.ds(base, STEP), :, pl.ds(pl.multiple_of(h * LANES, LANES), LANES)],
            ibuf.at[j % 2],
            i_sem.at[j % 2],
        )

    def turn(s):
        par = s % 2
        return xn + par * (yn - xn), yn + par * (xn - yn)

    def a_copy(s, j):
        h, g, k = place(s)
        n1, _ = turn(s)
        r = rows_of(k)
        block = dg if j == 0 else n1
        return rcopy(part.at[h, g, block, r], ra.at[h, g, j, r], a_send.at[s, j], a_recv.at[s, j], (n1, col))

    def b_copy(s):
        h, g, k = place(s)
        _, n2 = turn(s)
        r = rows_of(k)
        return rcopy(part.at[h, g, n2, r], rb.at[h, g, r], b_send.at[s], b_recv.at[s], (n2, col))

    def half_at(s, quarter):
        h, g, k = place(s)
        return half.at[
            h, pl.ds(g * GROUP, GROUP), pl.ds(pl.multiple_of(quarter * padded + k * STEP, STEP), STEP), :
        ]

    own_col = inner_i * core_col + (1 - inner_i) * pair_col

    def own_copy(s):
        ref = half_at(s, q)
        return rcopy(ref, ref, own_send.at[s], own_recv.at[1 - inner_i, s], (row, own_col))

    def own_arrival(s, kind, quarter):
        ref = half_at(s, quarter)
        return rcopy(ref, ref, own_send.at[s], own_recv.at[kind, s], (row, core_col))

    def fw_copy(s):
        ref = half_at(s, qo)
        return rcopy(ref, ref, fw_send.at[s], fw_recv.at[s], (row, core_col))

    def fw_arrival(s):
        ref = half_at(s, (zp % 2) * 2 + 1 - c)
        return rcopy(ref, ref, fw_send.at[s], fw_recv.at[s], (row, core_col))

    def v_core():
        return rcopy(vt_hbm.at[1 - c], vr.at[q], v_send.at[0], v_recv.at[q, 0], (row, core_col))

    def v_core_arrival():
        return rcopy(vt_hbm.at[1 - c], vr.at[qp], v_send.at[0], v_recv.at[qp, 0], (row, core_col))

    def v_local():
        return pltpu.make_async_copy(vt_hbm.at[c], vr.at[q], v_loc)

    def v_pair(core, side):
        start = far if side == 0 else near
        return rcopy(
            vt_hbm.at[core, pl.ds(start, 2)], vr.at[q, pl.ds(start, 2)],
            v_send.at[core * 2 + side], v_recv.at[q, side], (row, zp * 2 + core),
        )

    def v_pair_arrival(core, side):
        start = far if side == 0 else near
        src = (zp % 2) * 2 + core
        return rcopy(
            vt_hbm.at[core, pl.ds(start, 2)], vr.at[src, pl.ds(start, 2)],
            v_send.at[core * 2 + side], v_recv.at[src, side], (row, pair_col),
        )

    def unit(n):
        gr, m = n // units, n % units
        return gr // granules, gr % granules, m // 2, m % 2

    def product(h, g, pair, zb):
        acc = None
        i0 = g * GROUP + pair * 2
        for quarter in range(4):
            r = pl.ds(quarter * padded, padded)
            w = jnp.concatenate([half[h, i0, r, :], half[h, i0 + 1, r, :]], axis=1)
            term = jnp.dot(vr[quarter, zb], w, preferred_element_type=F32)
            acc = term if acc is None else acc + term
        return acc

    def q_copy(n):
        h, g, pair, b = unit(n)
        pi = g * pairs + pair
        return rcopy(qs.at[h, pi, b], qr.at[h, pi, b], q_send.at[n], q_recv.at[n], (row, mid_col))

    def out_at(n):
        h, g, pair, _ = unit(n)
        return out_hbm.at[pl.ds(g * GROUP + pair * 2, 2), :, pl.ds(pl.multiple_of(h * LANES, LANES), LANES)]

    def o_local(n):
        h, g, pair, _ = unit(n)
        return pltpu.make_async_copy(qr.at[h, g * pairs + pair, 0], out_at(n), l_sem.at[n // 2])

    def o_copy(n):
        h, g, pair, _ = unit(n)
        return rcopy(
            qr.at[h, g * pairs + pair, 1], out_at(n), o_send.at[n // 2], o_recv.at[n // 2], (row, pair_col)
        )

    def q_unit(n):
        h, g, pair, b = unit(n)
        pi = g * pairs + pair
        acc = product(h, g, pair, zm + b * (zmp - zm))
        qs[h, pi, b, 0] = acc[:, :LANES].astype(BF16)
        qs[h, pi, b, 1] = acc[:, LANES:].astype(BF16)
        q_copy(n).start()

    def s_unit(n):
        h, g, pair, b = unit(n)
        pi = g * pairs + pair
        q_copy(n).wait_recv()
        acc = product(h, g, pair, z + b * (zp - z))
        qr[h, pi, b, 0] = (acc[:, :LANES] + qr[h, pi, b, 0].astype(F32)).astype(BF16)
        qr[h, pi, b, 1] = (acc[:, LANES:] + qr[h, pi, b, 1].astype(F32)).astype(BF16)

        @pl.when(b == 0)
        def _():
            o_local(n).start()

        @pl.when(b == 1)
        def _():
            o_copy(n).start()

    chunk(0).start()

    @pl.when(inner)
    def _():
        v_local().start()
        v_core().start()

    @pl.when(outer)
    def _():
        v_pair(0, 0).start()
        v_pair(1, 0).start()

    n_chunks = blocks * steps

    def compute(j):
        h, k = j // steps, j % steps
        slot = j % 2
        chunk(j).wait()

        @pl.when(j + 1 < n_chunks)
        def _():
            chunk(j + 1).start()

        def couple(u, carry):
            w = jnp.concatenate([ibuf[slot, 2 * u], ibuf[slot, 2 * u + 1]], axis=1)
            r = jnp.dot(occ_ref[...], w, preferred_element_type=F32)
            cells = r.shape[0] // GROUP
            r0 = r[:, :LANES].reshape(cells, 1, GROUP, LANES)
            r1 = r[:, LANES:].reshape(cells, 1, GROUP, LANES)
            v = jnp.concatenate([r0, r1], axis=1).reshape(granules, 4, 2 * GROUP, LANES).astype(BF16)
            at = pl.multiple_of(k * rows_step + u * 2 * GROUP, 2 * GROUP)
            part[h, :, :, pl.ds(at, 2 * GROUP), :] = v
            return carry

        lax.fori_loop(0, STEP // 2, couple, 0, unroll=2)

    lag_f = LAG_B + 1
    lag_q = LAG_B + 2 + steps

    def iteration(t, carry):
        @pl.when(t < n_chunks)
        def _():
            compute(t)

        @pl.when(t < total)
        def _():
            for j in range(2):
                a_copy(t, j).start()

        s1 = t - LAG_A

        @pl.when((s1 >= 0) & (s1 < total))
        def _():
            h, g, k = place(s1)
            _, n2 = turn(s1)
            r = rows_of(k)
            a_copy(s1, 0).wait_recv()
            part[h, g, n2, r, :] = (part[h, g, n2, r, :].astype(F32) + ra[h, g, 0, r, :].astype(F32)).astype(BF16)
            b_copy(s1).start()

        s2 = t - LAG_B

        @pl.when((s2 >= 0) & (s2 < total))
        def _():
            h, g, k = place(s2)
            r = rows_of(k)
            a_copy(s2, 1).wait_recv()
            b_copy(s2).wait_recv()
            fsum[...] = (
                part[h, g, row, r, :].astype(F32) + ra[h, g, 1, r, :].astype(F32) + rb[h, g, r, :].astype(F32)
            )
            at = pl.multiple_of(q * padded + k * STEP, STEP)
            for i in range(GROUP):
                half[h, g * GROUP + i, pl.ds(at, STEP), :] = fsum[pl.ds(i, STEP, stride=GROUP), :].astype(BF16)
            own_copy(s2).start()

        @pl.when(outer & (t == steps + LAG_B))
        def _():
            v_pair(0, 1).start()
            v_pair(1, 1).start()

        tf = t - lag_f
        gf, uf = tf // steps, tf % steps

        @pl.when(inner & (tf >= 0) & (tf < total))
        def _():
            for j in range(2):
                kf = 2 * uf - (steps - 1) + j

                @pl.when((kf >= 0) & (kf < steps))
                def _():
                    s = gf * steps + kf
                    own_arrival(s, 1, qo).wait_recv()
                    fw_copy(s).start()

        tq = t - lag_q
        gq, uq = tq // steps, tq % steps

        @pl.when(inner & (tq == 0))
        def _():
            v_local().wait()
            v_core_arrival().wait_recv()
            v_pair_arrival(0, 0).wait_recv()
            v_pair_arrival(1, 0).wait_recv()

        @pl.when(inner & (tq >= 0) & (tq < total) & (uq == 0))
        def _():
            def arrivals(k, inner_carry):
                s = gq * steps + k
                own_arrival(s, 0, qp).wait_recv()
                fw_arrival(s).wait_recv()
                return inner_carry

            lax.fori_loop(0, steps, arrivals, 0)

        @pl.when(inner & (tq >= 0) & (tq < total) & (uq < units))
        def _():
            q_unit(gq * units + uq)

        gs = gq - LAG_S

        @pl.when(inner & (tq >= 0) & (gs == 0) & (uq == units))
        def _():
            v_pair_arrival(0, 1).wait_recv()
            v_pair_arrival(1, 1).wait_recv()

        @pl.when(inner & (tq >= 0) & (tq < total) & (gs >= 0) & (uq >= units) & (uq < 2 * units))
        def _():
            s_unit(gs * units + uq - units)

        return carry

    lax.fori_loop(0, total + LAG_B + 2 + units, iteration, 0)

    n_units = blocks * granules * units
    done_units = (blocks * granules - 1 - LAG_S) * units

    @pl.when(inner)
    def _():
        def finish(n, carry):
            s_unit(n)
            return carry

        lax.fori_loop(done_units, n_units, finish, 0)

        def drain(s, carry):
            fw_copy(s).wait_send()
            return carry

        lax.fori_loop(0, total, drain, 0)

        def drain_units(n, carry):
            q_copy(n).wait_send()

            @pl.when(n % 2 == 0)
            def _():
                o_local(n).wait()
                o_copy(n).wait_send()

            return carry

        lax.fori_loop(0, n_units, drain_units, 0)
        v_core().wait_send()

    @pl.when(outer)
    def _():
        def outputs(n, carry):
            o_copy(2 * n).wait_recv()
            return carry

        lax.fori_loop(0, n_units // 2, outputs, 0)
        for core in range(2):
            for side in range(2):
                v_pair(core, side).wait_send()

    def drain_all(s, carry):
        for j in range(2):
            a_copy(s, j).wait_send()
        b_copy(s).wait_send()
        own_copy(s).wait_send()
        return carry

    lax.fori_loop(0, total, drain_all, 0)


def fused(integrals, occ_coef, virt_coef, pair_index):
    rows, cols = lax.axis_size("row"), lax.axis_size("col")
    mus, nus, n_pairs = integrals.shape
    occ = occ_coef.shape[1]
    virt = virt_coef.shape[1]
    depth, width = occ // rows, virt // cols
    granules, blocks = depth // GROUP, n_pairs // LANES
    steps = -(-nus // STEP)
    padded = steps * STEP
    tail = padded - STEP
    total = blocks * granules * steps
    n_units = blocks * granules * GROUP
    halves = GROUP // 2 * granules

    flipped = jnp.transpose(integrals, (1, 0, 2))
    occ_rows = occ_coef.reshape(mus, rows, granules, GROUP).transpose(2, 1, 3, 0).reshape(occ, mus)
    spread = jnp.concatenate(
        [virt_coef[:tail], jnp.zeros((padded - nus, virt), BF16), virt_coef[tail:]], axis=0
    )
    columns = spread.reshape(padded, cols // 2, 2, width).transpose(2, 1, 3, 0)

    dma = pltpu.SemaphoreType.DMA
    r = padded * GROUP
    slab = pl.pallas_call(
        functools.partial(kernel, (nus, steps, blocks, granules)),
        out_shape=jax.ShapeDtypeStruct((depth, width, n_pairs), BF16),
        in_specs=[
            pl.BlockSpec(memory_space=pl.ANY),
            pl.BlockSpec(memory_space=pltpu.VMEM),
            pl.BlockSpec(memory_space=pl.ANY),
        ],
        out_specs=pl.BlockSpec(memory_space=pl.ANY),
        scratch_shapes=[
            pltpu.VMEM((2, STEP, mus, LANES), BF16),
            pltpu.VMEM((blocks, granules, rows, r, LANES), BF16),
            pltpu.VMEM((blocks, granules, 2, r, LANES), BF16),
            pltpu.VMEM((blocks, granules, r, LANES), BF16),
            pltpu.VMEM((blocks, depth, 4 * padded, LANES), BF16),
            pltpu.VMEM((4, cols // 2, width, padded), BF16),
            pltpu.VMEM((blocks, halves, 2, 2, width, LANES), BF16),
            pltpu.VMEM((blocks, halves, 2, 2, width, LANES), BF16),
            pltpu.VMEM((STEP * GROUP, LANES), F32),
            dma((2,)),
            dma((total, 2)), dma((total, 2)),
            dma((total,)), dma((total,)),
            dma((total,)), dma((2, total)),
            dma((total,)), dma((total,)),
            dma((n_units,)), dma((n_units,)),
            dma((n_units // 2,)), dma((n_units // 2,)), dma((n_units // 2,)),
            dma((4,)), dma((4, 2)), dma,
        ],
        compiler_params=pltpu.CompilerParams(
            collective_id=0, has_side_effects=True, vmem_limit_bytes=67043328
        ),
        name="half_transform",
    )(flipped, occ_rows, columns)
    chosen = (lax.broadcasted_iota(jnp.int32, (n_pairs, n_pairs), 0) == pair_index[None, :]).astype(BF16)
    return jnp.einsum("iap,pk->iak", slab, chosen, preferred_element_type=F32).astype(BF16)


CHUNKS = 2


def plain(integrals, occ_coef, virt_coef, pair_index):
    rows = lax.axis_size("row")
    mus, occ = occ_coef.shape
    virt_all = lax.all_gather(virt_coef, "col", axis=0, tiled=True)
    depth = occ // rows // CHUNKS
    occ_parts = occ_coef.reshape(mus, rows, CHUNKS, depth)
    outs = []
    for c in range(CHUNKS):
        part = jnp.einsum(
            "mri,mnp->rinp", occ_parts[:, :, c], integrals, preferred_element_type=F32
        ).astype(BF16)
        parts = lax.all_to_all(part, "row", split_axis=0, concat_axis=0, tiled=True)
        half = jnp.sum(parts.astype(F32), axis=0).astype(BF16)
        spread = lax.all_to_all(half, "col", split_axis=2, concat_axis=1, tiled=True)
        slab = jnp.einsum(
            "inp,na->iap", spread, virt_all, preferred_element_type=F32
        ).astype(BF16)
        outs.append(lax.all_to_all(slab, "col", split_axis=1, concat_axis=2, tiled=True))
    return jnp.take(jnp.concatenate(outs, axis=0), pair_index, axis=2)


def local(integrals, occ_coef, virt_coef, pair_index):
    rows, cols = lax.axis_size("row"), lax.axis_size("col")
    fits = (
        rows == SIDES**2
        and cols == SIDES**3
        and integrals.shape[1] >= STEP
        and integrals.shape[2] % LANES == 0
        and occ_coef.shape[1] % (rows * GROUP) == 0
        and virt_coef.shape[1] % (cols * 16) == 0
    )
    form = fused if fits else plain
    return form(integrals, occ_coef, virt_coef, pair_index)


def solution(mesh):
    return jax.shard_map(
        local,
        mesh=mesh,
        in_specs=(P("row", "col", None), P("row", None), P("col", None), P()),
        out_specs=P("row", "col", None),
        check_vma=False,
    )
```

```python
import functools

import jax
import jax.numpy as jnp
from jax import lax
from jax.experimental import pallas as pl
from jax.experimental.pallas import tpu as pltpu
from jax.sharding import PartitionSpec as P

MESH = pl.DeviceIdType.MESH
F32 = jnp.float32
BF16 = jnp.bfloat16

LANES = 128
GROUP = 8
STEP = 16
SIDES = 2
LAG_A = 4
LAG_B = 8
LAG_S = 1
RING = 20
BATCH = 4


def kernel(
    dims,
    x_hbm, occ_ref, vt_hbm, out_hbm,
    ibuf, part, ra, rb, half, vr, qs, qr, fsum,
    i_sem, a_send, a_recv, b_send, b_recv, own_send, own_recv, fw_send, fw_recv,
    q_send, q_recv, o_send, o_recv, l_sem, v_send, v_recv, v_loc,
):
    nus, steps, blocks, granules = dims
    padded = steps * STEP
    per_block = granules * steps
    total = blocks * per_block
    pairs = GROUP // 2
    units = pairs
    rows_step = STEP * GROUP

    row, col = lax.axis_index("row"), lax.axis_index("col")
    y, x = row // 2, row % 2
    z, c = col // 2, col % 2
    xn, yn, dg = row + 1 - 2 * x, row + 2 - 4 * y, 3 - row
    inner_i = (z % 2 + z // 2) % 2
    inner = inner_i == 1
    outer = inner_i == 0
    zp = z + 1 - 2 * (z % 2)
    zm = 3 - z
    core_col = col + 1 - 2 * c
    pair_col = zp * 2 + c
    mid_col = zm * 2 + c
    q = (z % 2) * 2 + c
    qp = (z % 2) * 2 + 1 - c
    qo = (zp % 2) * 2 + c
    far = (1 - z // 2) * 2
    near = (z // 2) * 2

    def rcopy(src, dst, ssem, rsem, dev):
        return pltpu.make_async_remote_copy(
            src_ref=src, dst_ref=dst, send_sem=ssem, recv_sem=rsem, device_id=dev, device_id_type=MESH
        )

    barrier = pltpu.get_barrier_semaphore()
    peers = (
        (xn, col), (yn, col), (row, core_col), (row, pair_col), (row, zp * 2 + 1 - c), (row, mid_col),
    )
    for dev in peers:
        pl.semaphore_signal(barrier, inc=1, device_id=dev, device_id_type=MESH)
    pl.semaphore_wait(barrier, len(peers))

    def place(s):
        h = s // per_block
        rem = s % per_block
        return h, rem // steps, rem % steps

    def rows_of(k):
        return pl.ds(pl.multiple_of(k * rows_step, rows_step), rows_step)

    def chunk(j):
        h, k = j // steps, j % steps
        base = jnp.minimum(k * STEP, nus - STEP)
        return pltpu.make_async_copy(
            x_hbm.at[pl.ds(base, STEP), :, pl.ds(pl.multiple_of(h * LANES, LANES), LANES)],
            ibuf.at[j % 2],
            i_sem.at[j % 2],
        )

    def turn(s):
        par = s % 2
        return xn + par * (yn - xn), yn + par * (xn - yn)

    def a_copy(s, j):
        h, g, k = place(s)
        n1, _ = turn(s)
        r = rows_of(k)
        block = dg if j == 0 else n1
        return rcopy(part.at[h, g, block, r], ra.at[h, g, j, r], a_send.at[j], a_recv.at[s % RING, j], (n1, col))

    def b_copy(s):
        h, g, k = place(s)
        _, n2 = turn(s)
        r = rows_of(k)
        return rcopy(part.at[h, g, n2, r], rb.at[h, g, r], b_send, b_recv.at[s % RING], (n2, col))

    def half_at(gr, first, count, quarter):
        h, g = gr // granules, gr % granules
        at = pl.multiple_of(quarter * padded + first * STEP, STEP)
        return half.at[h, pl.ds(g * GROUP, GROUP), pl.ds(at, count * STEP), :]

    own_col = inner_i * core_col + (1 - inner_i) * pair_col
    batches = [(b, min(BATCH, steps - b)) for b in range(0, steps, BATCH)]

    def own_copy(s):
        gr, k = s // steps, s % steps
        ref = half_at(gr, k, 1, q)
        slot = (1 - inner_i) * (1 + k // BATCH)
        return rcopy(ref, ref, own_send, own_recv.at[gr, slot], (row, own_col))

    def own_batch(gr, b):
        ref = half_at(gr, *batches[b], qo)
        return rcopy(ref, ref, own_send, own_recv.at[gr, 1 + b], (row, core_col))

    def own_arrival(gr):
        ref = half_at(gr, 0, steps, qp)
        return rcopy(ref, ref, own_send, own_recv.at[gr, 0], (row, core_col))

    def fw_copy(gr, b):
        ref = half_at(gr, *batches[b], qo)
        return rcopy(ref, ref, fw_send, fw_recv.at[gr], (row, core_col))

    def fw_arrival(gr):
        ref = half_at(gr, 0, steps, (zp % 2) * 2 + 1 - c)
        return rcopy(ref, ref, fw_send, fw_recv.at[gr], (row, core_col))

    def quarter_of(which):
        return half.at[:, :, pl.ds(pl.multiple_of(which * padded, STEP), padded), :]

    def v_core():
        return rcopy(vt_hbm.at[:, 1 - c], vr.at[q], v_send.at[0], v_recv.at[q, 0], (row, core_col))

    def v_core_arrival():
        return rcopy(vt_hbm.at[:, 1 - c], vr.at[qp], v_send.at[0], v_recv.at[qp, 0], (row, core_col))

    def v_local():
        return pltpu.make_async_copy(vt_hbm.at[:, c], vr.at[q], v_loc)

    def v_pair(core, side):
        start = far if side == 0 else near
        return rcopy(
            vt_hbm.at[pl.ds(start, 2), core], vr.at[q, pl.ds(start, 2)],
            v_send.at[core * 2 + side], v_recv.at[q, side], (row, zp * 2 + core),
        )

    def v_pair_arrival(core, side):
        start = far if side == 0 else near
        src = (zp % 2) * 2 + core
        return rcopy(
            vt_hbm.at[pl.ds(start, 2), core], vr.at[src, pl.ds(start, 2)],
            v_send.at[core * 2 + side], v_recv.at[src, side], (row, pair_col),
        )

    def unit(n):
        gr, pair = n // units, n % units
        return gr // granules, gr % granules, pair

    def product(h, g, pair, start):
        acc = None
        i0 = g * GROUP + pair * 2
        for quarter in range(4):
            r = pl.ds(quarter * padded, padded)
            w = jnp.concatenate([half[h, i0, r, :], half[h, i0 + 1, r, :]], axis=1)
            coef = vr[quarter, pl.ds(start, 2)]
            term = jnp.dot(coef.reshape(-1, padded), w, preferred_element_type=F32)
            acc = term if acc is None else acc + term
        return acc.reshape(2, -1, 2 * LANES)

    def q_copy(n):
        h, g, pair = unit(n)
        pi = g * pairs + pair
        return rcopy(qs.at[h, pi], qr.at[h, pi], q_send, q_recv.at[n], (row, mid_col))

    def out_at(n):
        h, g, pair = unit(n)
        return out_hbm.at[pl.ds(g * GROUP + pair * 2, 2), :, pl.ds(pl.multiple_of(h * LANES, LANES), LANES)]

    def o_local(n):
        h, g, pair = unit(n)
        return pltpu.make_async_copy(qr.at[h, g * pairs + pair, z % 2], out_at(n), l_sem)

    def o_copy(n):
        h, g, pair = unit(n)
        return rcopy(qr.at[h, g * pairs + pair, zp % 2], out_at(n), o_send, o_recv, (row, pair_col))

    def q_unit(n):
        h, g, pair = unit(n)
        pi = g * pairs + pair
        acc = product(h, g, pair, far)
        for j in range(2):
            qs[h, pi, :, j] = acc[:, :, j * LANES:(j + 1) * LANES].astype(BF16)
        q_copy(n).start()

    def s_unit(n):
        h, g, pair = unit(n)
        pi = g * pairs + pair
        q_copy(n).wait_recv()
        acc = product(h, g, pair, near)
        for j in range(2):
            total_j = acc[:, :, j * LANES:(j + 1) * LANES] + qr[h, pi, :, j].astype(F32)
            qr[h, pi, :, j] = total_j.astype(BF16)
        o_copy(n).start()
        o_local(n).start()

    chunk(0).start()

    @pl.when(inner)
    def _():
        v_local().start()
        v_core().start()

    @pl.when(outer)
    def _():
        v_pair(0, 0).start()
        v_pair(1, 0).start()

    n_chunks = blocks * steps

    def compute(j):
        h, k = j // steps, j % steps
        slot = j % 2

        @pl.when(j + 1 < n_chunks)
        def _():
            chunk(j + 1).start()

        chunk(j).wait()

        def couple(u, carry):
            w = jnp.concatenate([ibuf[slot, 2 * u], ibuf[slot, 2 * u + 1]], axis=1)
            r = jnp.dot(occ_ref[...], w, preferred_element_type=F32)
            cells = r.shape[0] // GROUP
            r0 = r[:, :LANES].reshape(cells, 1, GROUP, LANES)
            r1 = r[:, LANES:].reshape(cells, 1, GROUP, LANES)
            v = jnp.concatenate([r0, r1], axis=1).reshape(4, granules, 2 * GROUP, LANES).astype(BF16)
            at = pl.multiple_of(k * rows_step + u * 2 * GROUP, 2 * GROUP)
            for o in range(4):
                part[h, :, o, pl.ds(at, 2 * GROUP), :] = v[o]
            return carry

        lax.fori_loop(0, STEP // 2, couple, 0, unroll=STEP // 2)

    s_every = max((steps - 1) // (2 * units), 1)
    s_first = steps - 1 - s_every * (units - 1)
    lag_f = LAG_B + 3
    lag_q = LAG_B + 4 + steps
    spread = max((per_block + steps - 1 - lag_q) // (steps - 1), 1)

    def iteration(t, carry):
        past = t - lag_q
        ready = jnp.where(t < steps, t, steps + past // spread)

        @pl.when((t < steps) | ((past >= 0) & (past % spread == 0) & (ready < n_chunks)))
        def _():
            compute(ready)

        @pl.when(t < total)
        def _():
            for j in range(2):
                a_copy(t, j).start()

        s1 = t - LAG_A

        @pl.when((s1 >= 0) & (s1 < total))
        def _():
            h, g, k = place(s1)
            _, n2 = turn(s1)
            r = rows_of(k)
            a_copy(s1, 0).wait_recv()
            part[h, g, n2, r, :] = (part[h, g, n2, r, :].astype(F32) + ra[h, g, 0, r, :].astype(F32)).astype(BF16)
            b_copy(s1).start()

        s2 = t - LAG_B

        @pl.when((s2 >= 0) & (s2 < total))
        def _():
            h, g, k = place(s2)
            r = rows_of(k)
            a_copy(s2, 1).wait_recv()
            b_copy(s2).wait_recv()
            fsum[...] = (
                part[h, g, row, r, :].astype(F32) + ra[h, g, 1, r, :].astype(F32) + rb[h, g, r, :].astype(F32)
            )
            at = pl.multiple_of(q * padded + k * STEP, STEP)
            for i in range(GROUP):
                half[h, g * GROUP + i, pl.ds(at, STEP), :] = fsum[pl.ds(i, STEP, stride=GROUP), :].astype(BF16)
            own_copy(s2).start()

        @pl.when(outer & (t == steps + LAG_B))
        def _():
            v_pair(0, 1).start()
            v_pair(1, 1).start()

        tf = t - lag_f
        gf, uf = tf // steps, tf % steps

        @pl.when(inner & (tf >= 0) & (tf < total))
        def _():
            for b in range(len(batches)):

                @pl.when(uf == steps - 1 - 2 * (len(batches) - 1 - b))
                def _():
                    own_batch(gf, b).wait_recv()
                    fw_copy(gf, b).start()

        tq = t - lag_q
        gq, uq = tq // steps, tq % steps

        @pl.when(inner & (tq == 0))
        def _():
            v_local().wait()
            v_core_arrival().wait_recv()
            v_pair_arrival(0, 0).wait_recv()
            v_pair_arrival(1, 0).wait_recv()

        @pl.when(inner & (tq >= 0) & (tq < total) & (uq == 0))
        def _():
            own_arrival(gq).wait_recv()
            fw_arrival(gq).wait_recv()

        @pl.when(inner & (tq >= 0) & (tq < total) & (uq < units))
        def _():
            q_unit(gq * units + uq)

        gs = gq - LAG_S

        @pl.when(inner & (tq >= 0) & (gs == 0) & (uq == s_first))
        def _():
            v_pair_arrival(0, 1).wait_recv()
            v_pair_arrival(1, 1).wait_recv()

        us = uq - s_first

        @pl.when(inner & (tq >= 0) & (tq < total) & (gs >= 0) & (us >= 0) & (us % s_every == 0) & (us // s_every < units))
        def _():
            s_unit(gs * units + us // s_every)

        return carry

    lax.fori_loop(0, total + lag_q - steps + units, iteration, 0)

    n_units = blocks * granules * units
    done_units = (blocks * granules - 1 - LAG_S) * units

    @pl.when(inner)
    def _():
        def finish(n, carry):
            s_unit(n)
            return carry

        lax.fori_loop(done_units, n_units, finish, 0)

        rcopy(quarter_of(qo), quarter_of(qo), fw_send, fw_recv.at[0], (row, core_col)).wait_send()
        rcopy(qs, qr, q_send, q_recv.at[0], (row, mid_col)).wait_send()
        rcopy(out_hbm, out_hbm, o_send, o_recv, (row, pair_col)).wait_send()
        pltpu.make_async_copy(out_hbm, out_hbm, l_sem).wait()
        v_core().wait_send()

    @pl.when(outer)
    def _():
        rcopy(out_hbm, out_hbm, o_send, o_recv, (row, pair_col)).wait_recv()
        for core in range(2):
            for side in range(2):
                v_pair(core, side).wait_send()

    for j in range(2):
        rcopy(ra.at[:, :, j], ra.at[:, :, j], a_send.at[j], a_recv.at[0, j], (xn, col)).wait_send()
    rcopy(rb, rb, b_send, b_recv.at[0], (yn, col)).wait_send()
    rcopy(quarter_of(q), quarter_of(q), own_send, own_recv.at[0, 0], (row, own_col)).wait_send()


def fused(integrals, occ_coef, virt_coef, pair_index):
    rows, cols = lax.axis_size("row"), lax.axis_size("col")
    mus, nus, n_pairs = integrals.shape
    occ = occ_coef.shape[1]
    virt = virt_coef.shape[1]
    depth, width = occ // rows, virt // cols
    granules, blocks = depth // GROUP, n_pairs // LANES
    steps = -(-nus // STEP)
    padded = steps * STEP
    tail = padded - STEP
    n_units = blocks * granules * (GROUP // 2)
    halves = GROUP // 2 * granules

    flipped = jnp.transpose(integrals, (1, 0, 2))
    spread = jnp.concatenate(
        [virt_coef[:tail], jnp.zeros((padded - nus, virt), BF16), virt_coef[tail:]], axis=0
    )
    columns = spread.T.reshape(cols // 2, 2, width, padded)

    dma = pltpu.SemaphoreType.DMA
    r = padded * GROUP
    slab = pl.pallas_call(
        functools.partial(kernel, (nus, steps, blocks, granules)),
        out_shape=jax.ShapeDtypeStruct((depth, width, n_pairs), BF16),
        in_specs=[
            pl.BlockSpec(memory_space=pl.ANY),
            pl.BlockSpec(memory_space=pltpu.VMEM),
            pl.BlockSpec(memory_space=pl.ANY),
        ],
        out_specs=pl.BlockSpec(memory_space=pl.ANY),
        scratch_shapes=[
            pltpu.VMEM((2, STEP, mus, LANES), BF16),
            pltpu.VMEM((blocks, granules, rows, r, LANES), BF16),
            pltpu.VMEM((blocks, granules, 2, r, LANES), BF16),
            pltpu.VMEM((blocks, granules, r, LANES), BF16),
            pltpu.VMEM((blocks, depth, 4 * padded, LANES), BF16),
            pltpu.VMEM((4, cols // 2, width, padded), BF16),
            pltpu.VMEM((blocks, halves, 2, 2, width, LANES), BF16),
            pltpu.VMEM((blocks, halves, 2, 2, width, LANES), BF16),
            pltpu.VMEM((STEP * GROUP, LANES), F32),
            dma((2,)),
            dma((2,)), dma((RING, 2)),
            dma, dma((RING,)),
            dma, dma((blocks * granules, 1 + -(-steps // BATCH))),
            dma, dma((blocks * granules,)),
            dma, dma((n_units,)),
            dma, dma, dma,
            dma((4,)), dma((4, 2)), dma,
        ],
        compiler_params=pltpu.CompilerParams(
            collective_id=0, has_side_effects=True, vmem_limit_bytes=67043328
        ),
        name="half_transform",
    )(flipped, occ_coef.T, columns)
    chosen = (lax.broadcasted_iota(jnp.int32, (n_pairs, n_pairs), 0) == pair_index[None, :]).astype(BF16)
    return jnp.einsum("iap,pk->iak", slab, chosen, preferred_element_type=F32).astype(BF16)


CHUNKS = 2


def plain(integrals, occ_coef, virt_coef, pair_index):
    rows = lax.axis_size("row")
    mus, occ = occ_coef.shape
    virt_all = lax.all_gather(virt_coef, "col", axis=0, tiled=True)
    depth = occ // rows // CHUNKS
    occ_parts = occ_coef.reshape(mus, rows, CHUNKS, depth)
    outs = []
    for c in range(CHUNKS):
        part = jnp.einsum(
            "mri,mnp->rinp", occ_parts[:, :, c], integrals, preferred_element_type=F32
        ).astype(BF16)
        parts = lax.all_to_all(part, "row", split_axis=0, concat_axis=0, tiled=True)
        half = jnp.sum(parts.astype(F32), axis=0).astype(BF16)
        spread = lax.all_to_all(half, "col", split_axis=2, concat_axis=1, tiled=True)
        slab = jnp.einsum(
            "inp,na->iap", spread, virt_all, preferred_element_type=F32
        ).astype(BF16)
        outs.append(lax.all_to_all(slab, "col", split_axis=1, concat_axis=2, tiled=True))
    return jnp.take(jnp.concatenate(outs, axis=0), pair_index, axis=2)


def local(integrals, occ_coef, virt_coef, pair_index):
    rows, cols = lax.axis_size("row"), lax.axis_size("col")
    fits = (
        rows == SIDES**2
        and cols == SIDES**3
        and integrals.shape[1] >= STEP
        and integrals.shape[2] == 2 * LANES
        and occ_coef.shape[1] % (rows * GROUP) == 0
        and virt_coef.shape[1] % (cols * 16) == 0
    )
    form = fused if fits else plain
    return form(integrals, occ_coef, virt_coef, pair_index)


def solution(mesh):
    return jax.shard_map(
        local,
        mesh=mesh,
        in_specs=(P("row", "col", None), P("row", None), P("col", None), P()),
        out_specs=P("row", "col", None),
        check_vma=False,
    )
```

```python
import functools

import jax
import jax.numpy as jnp
from jax import lax
from jax.experimental import pallas as pl
from jax.experimental.pallas import tpu as pltpu
from jax.sharding import PartitionSpec as P

MESH = pl.DeviceIdType.MESH
F32 = jnp.float32
BF16 = jnp.bfloat16

LANES = 128
GROUP = 8
STEP = 16
SIDES = 2
LAG_A = 4
LAG_B = 8
LAG_S = 1
RING = 20
V_FIRST = 28
V_EVERY = 4
BATCH = 4


def kernel(
    dims,
    x_hbm, occ_ref, vt_hbm, out_hbm,
    ibuf, part, ra, rb, half, vr, qs, qr, fsum,
    i_sem, a_send, a_recv, b_send, b_recv, own_send, own_recv, fw_send, fw_recv,
    q_send, q_recv, o_send, o_recv, l_sem, v_send, v_recv, v_loc,
):
    nus, steps, blocks, granules = dims
    padded = steps * STEP
    per_block = granules * steps
    total = blocks * per_block
    pairs = GROUP // 2
    units = pairs
    rows_step = STEP * GROUP

    row, col = lax.axis_index("row"), lax.axis_index("col")
    y, x = row // 2, row % 2
    z, c = col // 2, col % 2
    xn, yn, dg = row + 1 - 2 * x, row + 2 - 4 * y, 3 - row
    inner_i = (z % 2 + z // 2) % 2
    inner = inner_i == 1
    outer = inner_i == 0
    zp = z + 1 - 2 * (z % 2)
    zm = 3 - z
    core_col = col + 1 - 2 * c
    pair_col = zp * 2 + c
    mid_col = zm * 2 + c
    q = (z % 2) * 2 + c
    qp = (z % 2) * 2 + 1 - c
    qo = (zp % 2) * 2 + c
    far = (1 - z // 2) * 2
    near = (z // 2) * 2

    def rcopy(src, dst, ssem, rsem, dev):
        return pltpu.make_async_remote_copy(
            src_ref=src, dst_ref=dst, send_sem=ssem, recv_sem=rsem, device_id=dev, device_id_type=MESH
        )

    barrier = pltpu.get_barrier_semaphore()
    peers = (
        (xn, col), (yn, col), (row, core_col), (row, pair_col), (row, zp * 2 + 1 - c), (row, mid_col),
    )
    for dev in peers:
        pl.semaphore_signal(barrier, inc=1, device_id=dev, device_id_type=MESH)
    pl.semaphore_wait(barrier, len(peers))

    def place(s):
        h = s // per_block
        rem = s % per_block
        return h, rem // steps, rem % steps

    def rows_of(k):
        return pl.ds(pl.multiple_of(k * rows_step, rows_step), rows_step)

    def chunk(j):
        h, k = j // steps, j % steps
        base = jnp.minimum(k * STEP, nus - STEP)
        return pltpu.make_async_copy(
            x_hbm.at[pl.ds(base, STEP), :, pl.ds(pl.multiple_of(h * LANES, LANES), LANES)],
            ibuf.at[j % 2],
            i_sem.at[j % 2],
        )

    def turn(s):
        par = s % 2
        return xn + par * (yn - xn), yn + par * (xn - yn)

    def a_copy(s, j):
        h, g, k = place(s)
        n1, _ = turn(s)
        r = rows_of(k)
        block = dg if j == 0 else n1
        return rcopy(part.at[h, g, block, r], ra.at[h, g, j, r], a_send.at[j], a_recv.at[s % RING, j], (n1, col))

    def b_copy(s):
        h, g, k = place(s)
        _, n2 = turn(s)
        r = rows_of(k)
        return rcopy(part.at[h, g, n2, r], rb.at[h, g, r], b_send, b_recv.at[s % RING], (n2, col))

    def half_at(gr, first, count, quarter):
        h, g = gr // granules, gr % granules
        at = pl.multiple_of(quarter * padded + first * STEP, STEP)
        return half.at[h, pl.ds(g * GROUP, GROUP), pl.ds(at, count * STEP), :]

    own_col = inner_i * core_col + (1 - inner_i) * pair_col
    batches = [(b, min(BATCH, steps - b)) for b in range(0, steps, BATCH)]

    def own_copy(s):
        gr, k = s // steps, s % steps
        ref = half_at(gr, k, 1, q)
        slot = (1 - inner_i) * (1 + k // BATCH)
        return rcopy(ref, ref, own_send, own_recv.at[gr, slot], (row, own_col))

    def own_batch(gr, b):
        ref = half_at(gr, *batches[b], qo)
        return rcopy(ref, ref, own_send, own_recv.at[gr, 1 + b], (row, core_col))

    def own_arrival(gr):
        ref = half_at(gr, 0, steps, qp)
        return rcopy(ref, ref, own_send, own_recv.at[gr, 0], (row, core_col))

    def fw_copy(gr, b):
        ref = half_at(gr, *batches[b], qo)
        return rcopy(ref, ref, fw_send, fw_recv.at[gr], (row, core_col))

    def fw_arrival(gr):
        ref = half_at(gr, 0, steps, (zp % 2) * 2 + 1 - c)
        return rcopy(ref, ref, fw_send, fw_recv.at[gr], (row, core_col))

    def quarter_of(which):
        return half.at[:, :, pl.ds(pl.multiple_of(which * padded, STEP), padded), :]

    def v_core():
        return rcopy(vt_hbm.at[:, 1 - c], vr.at[q], v_send.at[0], v_recv.at[q, 0], (row, core_col))

    def v_core_arrival():
        return rcopy(vt_hbm.at[:, 1 - c], vr.at[qp], v_send.at[0], v_recv.at[qp, 0], (row, core_col))

    def v_local():
        return pltpu.make_async_copy(vt_hbm.at[:, c], vr.at[q], v_loc)

    def v_pair(core, side):
        start = far if side == 0 else near
        return rcopy(
            vt_hbm.at[pl.ds(start, 2), core], vr.at[q, pl.ds(start, 2)],
            v_send.at[core * 2 + side], v_recv.at[q, side], (row, zp * 2 + core),
        )

    def v_piece(n):
        core, part_of = n // 4, n % 4
        at = near + part_of // 2
        rows_half = vt_hbm.shape[2] // 2
        r = pl.ds(pl.multiple_of((part_of % 2) * rows_half, STEP), rows_half)
        return rcopy(
            vt_hbm.at[at, core, r], vr.at[q, at, r],
            v_send.at[core * 2 + 1], v_recv.at[q, 1], (row, zp * 2 + core),
        )

    def v_pair_arrival(core, side):
        start = far if side == 0 else near
        src = (zp % 2) * 2 + core
        return rcopy(
            vt_hbm.at[pl.ds(start, 2), core], vr.at[src, pl.ds(start, 2)],
            v_send.at[core * 2 + side], v_recv.at[src, side], (row, pair_col),
        )

    def unit(n):
        gr, pair = n // units, n % units
        return gr // granules, gr % granules, pair

    def product(h, g, pair, start):
        acc = None
        i0 = g * GROUP + pair * 2
        for quarter in range(4):
            r = pl.ds(quarter * padded, padded)
            w = jnp.concatenate([half[h, i0, r, :], half[h, i0 + 1, r, :]], axis=1)
            coef = vr[quarter, pl.ds(start, 2)]
            term = jnp.dot(coef.reshape(-1, padded), w, preferred_element_type=F32)
            acc = term if acc is None else acc + term
        return acc.reshape(2, -1, 2 * LANES)

    def q_copy(n):
        h, g, pair = unit(n)
        pi = g * pairs + pair
        return rcopy(qs.at[h, pi], qr.at[h, pi], q_send, q_recv.at[n], (row, mid_col))

    def out_at(n):
        h, g, pair = unit(n)
        return out_hbm.at[pl.ds(g * GROUP + pair * 2, 2), :, pl.ds(pl.multiple_of(h * LANES, LANES), LANES)]

    def o_local(n):
        h, g, pair = unit(n)
        return pltpu.make_async_copy(qr.at[h, g * pairs + pair, z % 2], out_at(n), l_sem)

    def o_copy(n):
        h, g, pair = unit(n)
        return rcopy(qr.at[h, g * pairs + pair, zp % 2], out_at(n), o_send, o_recv, (row, pair_col))

    def q_unit(n):
        h, g, pair = unit(n)
        pi = g * pairs + pair
        acc = product(h, g, pair, far)
        for j in range(2):
            qs[h, pi, :, j] = acc[:, :, j * LANES:(j + 1) * LANES].astype(BF16)
        q_copy(n).start()

    def s_unit(n):
        h, g, pair = unit(n)
        pi = g * pairs + pair
        q_copy(n).wait_recv()
        acc = product(h, g, pair, near)
        for j in range(2):
            total_j = acc[:, :, j * LANES:(j + 1) * LANES] + qr[h, pi, :, j].astype(F32)
            qr[h, pi, :, j] = total_j.astype(BF16)
        o_copy(n).start()
        o_local(n).start()

    chunk(0).start()

    @pl.when(inner)
    def _():
        v_local().start()
        v_core().start()

    @pl.when(outer)
    def _():
        v_pair(0, 0).start()
        v_pair(1, 0).start()

    n_chunks = blocks * steps

    def compute(j):
        h, k = j // steps, j % steps
        slot = j % 2

        @pl.when(j + 1 < n_chunks)
        def _():
            chunk(j + 1).start()

        chunk(j).wait()

        def couple(u, carry):
            w = jnp.concatenate([ibuf[slot, 2 * u], ibuf[slot, 2 * u + 1]], axis=1)
            r = jnp.dot(occ_ref[...], w, preferred_element_type=F32)
            cells = r.shape[0] // GROUP
            r0 = r[:, :LANES].reshape(cells, 1, GROUP, LANES)
            r1 = r[:, LANES:].reshape(cells, 1, GROUP, LANES)
            v = jnp.concatenate([r0, r1], axis=1).reshape(4, granules, 2 * GROUP, LANES).astype(BF16)
            at = pl.multiple_of(k * rows_step + u * 2 * GROUP, 2 * GROUP)
            for o in range(4):
                part[h, :, o, pl.ds(at, 2 * GROUP), :] = v[o]
            return carry

        lax.fori_loop(0, STEP // 2, couple, 0, unroll=STEP // 2)

    s_every = max((steps - 1) // (2 * units), 1)
    s_first = steps - 1 - s_every * (units - 1)
    lag_f = LAG_B + 3
    lag_q = LAG_B + 4 + steps
    spread = max((per_block + steps - 1 - lag_q) // (steps - 1), 1)

    def iteration(t, carry):
        past = t - lag_q
        ready = jnp.where(t < steps, t, steps + past // spread)

        @pl.when((t < steps) | ((past >= 0) & (past % spread == 0) & (ready < n_chunks)))
        def _():
            compute(ready)

        @pl.when(t < total)
        def _():
            for j in range(2):
                a_copy(t, j).start()

        s1 = t - LAG_A

        @pl.when((s1 >= 0) & (s1 < total))
        def _():
            h, g, k = place(s1)
            _, n2 = turn(s1)
            r = rows_of(k)
            a_copy(s1, 0).wait_recv()
            part[h, g, n2, r, :] = (part[h, g, n2, r, :].astype(F32) + ra[h, g, 0, r, :].astype(F32)).astype(BF16)
            b_copy(s1).start()

        s2 = t - LAG_B

        @pl.when((s2 >= 0) & (s2 < total))
        def _():
            h, g, k = place(s2)
            r = rows_of(k)
            a_copy(s2, 1).wait_recv()
            b_copy(s2).wait_recv()
            fsum[...] = (
                part[h, g, row, r, :].astype(F32) + ra[h, g, 1, r, :].astype(F32) + rb[h, g, r, :].astype(F32)
            )
            at = pl.multiple_of(q * padded + k * STEP, STEP)
            for i in range(GROUP):
                half[h, g * GROUP + i, pl.ds(at, STEP), :] = fsum[pl.ds(i, STEP, stride=GROUP), :].astype(BF16)
            own_copy(s2).start()

        tv = t - V_FIRST

        @pl.when(outer & (tv >= 0) & (tv % V_EVERY == 0) & (tv // V_EVERY < 8))
        def _():
            v_piece(tv // V_EVERY).start()

        tf = t - lag_f
        gf, uf = tf // steps, tf % steps

        @pl.when(inner & (tf >= 0) & (tf < total))
        def _():
            for b in range(len(batches)):

                @pl.when(uf == steps - 1 - 2 * (len(batches) - 1 - b))
                def _():
                    own_batch(gf, b).wait_recv()
                    fw_copy(gf, b).start()

        tq = t - lag_q
        gq, uq = tq // steps, tq % steps

        @pl.when(inner & (tq == 0))
        def _():
            v_local().wait()
            v_core_arrival().wait_recv()
            v_pair_arrival(0, 0).wait_recv()
            v_pair_arrival(1, 0).wait_recv()

        @pl.when(inner & (tq >= 0) & (tq < total) & (uq == 0))
        def _():
            own_arrival(gq).wait_recv()
            fw_arrival(gq).wait_recv()

        @pl.when(inner & (tq >= 0) & (tq < total) & (uq < units))
        def _():
            q_unit(gq * units + uq)

        gs = gq - LAG_S

        @pl.when(inner & (tq >= 0) & (gs == 0) & (uq == s_first))
        def _():
            v_pair_arrival(0, 1).wait_recv()
            v_pair_arrival(1, 1).wait_recv()

        us = uq - s_first

        @pl.when(inner & (tq >= 0) & (tq < total) & (gs >= 0) & (us >= 0) & (us % s_every == 0) & (us // s_every < units))
        def _():
            s_unit(gs * units + us // s_every)

        return carry

    lax.fori_loop(0, total + lag_q - steps + units, iteration, 0)

    n_units = blocks * granules * units
    done_units = (blocks * granules - 1 - LAG_S) * units

    @pl.when(inner)
    def _():
        def finish(n, carry):
            s_unit(n)
            return carry

        lax.fori_loop(done_units, n_units, finish, 0)

        rcopy(quarter_of(qo), quarter_of(qo), fw_send, fw_recv.at[0], (row, core_col)).wait_send()
        rcopy(qs, qr, q_send, q_recv.at[0], (row, mid_col)).wait_send()
        rcopy(out_hbm, out_hbm, o_send, o_recv, (row, pair_col)).wait_send()
        pltpu.make_async_copy(out_hbm, out_hbm, l_sem).wait()
        v_core().wait_send()

    @pl.when(outer)
    def _():
        rcopy(out_hbm, out_hbm, o_send, o_recv, (row, pair_col)).wait_recv()
        for core in range(2):
            for side in range(2):
                v_pair(core, side).wait_send()

    for j in range(2):
        rcopy(ra.at[:, :, j], ra.at[:, :, j], a_send.at[j], a_recv.at[0, j], (xn, col)).wait_send()
    rcopy(rb, rb, b_send, b_recv.at[0], (yn, col)).wait_send()
    rcopy(quarter_of(q), quarter_of(q), own_send, own_recv.at[0, 0], (row, own_col)).wait_send()


def fused(integrals, occ_coef, virt_coef, pair_index):
    rows, cols = lax.axis_size("row"), lax.axis_size("col")
    mus, nus, n_pairs = integrals.shape
    occ = occ_coef.shape[1]
    virt = virt_coef.shape[1]
    depth, width = occ // rows, virt // cols
    granules, blocks = depth // GROUP, n_pairs // LANES
    steps = -(-nus // STEP)
    padded = steps * STEP
    tail = padded - STEP
    n_units = blocks * granules * (GROUP // 2)
    halves = GROUP // 2 * granules

    flipped = jnp.transpose(integrals, (1, 0, 2))
    spread = jnp.concatenate(
        [virt_coef[:tail], jnp.zeros((padded - nus, virt), BF16), virt_coef[tail:]], axis=0
    )
    columns = spread.T.reshape(cols // 2, 2, width, padded)

    dma = pltpu.SemaphoreType.DMA
    r = padded * GROUP
    slab = pl.pallas_call(
        functools.partial(kernel, (nus, steps, blocks, granules)),
        out_shape=jax.ShapeDtypeStruct((depth, width, n_pairs), BF16),
        in_specs=[
            pl.BlockSpec(memory_space=pl.ANY),
            pl.BlockSpec(memory_space=pltpu.VMEM),
            pl.BlockSpec(memory_space=pl.ANY),
        ],
        out_specs=pl.BlockSpec(memory_space=pl.ANY),
        scratch_shapes=[
            pltpu.VMEM((2, STEP, mus, LANES), BF16),
            pltpu.VMEM((blocks, granules, rows, r, LANES), BF16),
            pltpu.VMEM((blocks, granules, 2, r, LANES), BF16),
            pltpu.VMEM((blocks, granules, r, LANES), BF16),
            pltpu.VMEM((blocks, depth, 4 * padded, LANES), BF16),
            pltpu.VMEM((4, cols // 2, width, padded), BF16),
            pltpu.VMEM((blocks, halves, 2, 2, width, LANES), BF16),
            pltpu.VMEM((blocks, halves, 2, 2, width, LANES), BF16),
            pltpu.VMEM((STEP * GROUP, LANES), F32),
            dma((2,)),
            dma((2,)), dma((RING, 2)),
            dma, dma((RING,)),
            dma, dma((blocks * granules, 1 + -(-steps // BATCH))),
            dma, dma((blocks * granules,)),
            dma, dma((n_units,)),
            dma, dma, dma,
            dma((4,)), dma((4, 2)), dma,
        ],
        compiler_params=pltpu.CompilerParams(
            collective_id=0, has_side_effects=True, vmem_limit_bytes=67043328
        ),
        name="half_transform",
    )(flipped, occ_coef.T, columns)
    chosen = (lax.broadcasted_iota(jnp.int32, (n_pairs, n_pairs), 0) == pair_index[None, :]).astype(BF16)
    return jnp.einsum("iap,pk->iak", slab, chosen, preferred_element_type=F32).astype(BF16)


CHUNKS = 2


def plain(integrals, occ_coef, virt_coef, pair_index):
    rows = lax.axis_size("row")
    mus, occ = occ_coef.shape
    virt_all = lax.all_gather(virt_coef, "col", axis=0, tiled=True)
    depth = occ // rows // CHUNKS
    occ_parts = occ_coef.reshape(mus, rows, CHUNKS, depth)
    outs = []
    for c in range(CHUNKS):
        part = jnp.einsum(
            "mri,mnp->rinp", occ_parts[:, :, c], integrals, preferred_element_type=F32
        ).astype(BF16)
        parts = lax.all_to_all(part, "row", split_axis=0, concat_axis=0, tiled=True)
        half = jnp.sum(parts.astype(F32), axis=0).astype(BF16)
        spread = lax.all_to_all(half, "col", split_axis=2, concat_axis=1, tiled=True)
        slab = jnp.einsum(
            "inp,na->iap", spread, virt_all, preferred_element_type=F32
        ).astype(BF16)
        outs.append(lax.all_to_all(slab, "col", split_axis=1, concat_axis=2, tiled=True))
    return jnp.take(jnp.concatenate(outs, axis=0), pair_index, axis=2)


def local(integrals, occ_coef, virt_coef, pair_index):
    rows, cols = lax.axis_size("row"), lax.axis_size("col")
    fits = (
        rows == SIDES**2
        and cols == SIDES**3
        and integrals.shape[1] >= STEP
        and integrals.shape[2] == 2 * LANES
        and occ_coef.shape[1] % (rows * GROUP) == 0
        and virt_coef.shape[1] % (cols * 2 * STEP) == 0
        and occ_coef.shape[1] // (rows * GROUP) * 2 * (integrals.shape[1] // STEP) > V_FIRST + 8 * V_EVERY
    )
    form = fused if fits else plain
    return form(integrals, occ_coef, virt_coef, pair_index)


def solution(mesh):
    return jax.shard_map(
        local,
        mesh=mesh,
        in_specs=(P("row", "col", None), P("row", None), P("col", None), P()),
        out_specs=P("row", "col", None),
        check_vma=False,
    )
```
